32 devices in a mesh: row: 4 (over z), col: 8 (over y, x, core).
Axes of the slice: x: 2, y: 2, z: 4, core: 2. Of those that a mesh axis runs over, the one named last changes fastest.
Arguments:
- slab_pair: float32 [65536, 4096], P('row', 'col'), may hold values from -6 to 6, as said below
- butterfly_scale: float32 [65536], P('row'), may hold values from 0.5 to 2
Outputs:
- transformed: float32 [65536, 4096], P('row', 'col')
The draws below stay inside these ranges and needn't reach their ends.
Inputs may be any that keep to these rules, and one draw needn't show every extreme that they name: The matrix is symmetric where the slab pair meets its own columns: with g(k) = k for k < 2048 and 32768 + k - 2048 otherwise, slab_pair[g(a), b] = slab_pair[g(b), a] for all a, b below 4096.
All inputs are finite; a program needn't handle non-finite values.
Results may differ from the reference program's by a relative error of at most 0.00002.
Values sent between devices are 32-bit elements; how exact they have to be, the bound alone decides.
A program may use at most 192 MiB of HBM per device.

```python
import math
import jax
import jax.numpy as jnp

N = 65536
W = 2048
HALF = 32768


def draw_slab_pair(key, part):
    base = jnp.clip(jax.random.normal(key, (N, 2 * W), jnp.float32), -6.0, 6.0)
    block = jnp.concatenate([base[:W], base[HALF:HALF + W]], axis=0)
    mirrored = jnp.clip((block + block.T) * jnp.float32(0.5) ** 0.5, -6.0, 6.0)
    base = base.at[:W].set(mirrored[:W])
    base = base.at[HALF:HALF + W].set(mirrored[W:])
    return base


def shard_levels(key, dims, pieces, smallest, largest):
    def one(axis_at, parts):
        steps = jax.random.uniform(jax.random.fold_in(jax.random.fold_in(key, 6), axis_at), (parts,), jnp.float32, smallest / len(pieces), largest / len(pieces))
        return jnp.repeat(jnp.exp(steps), dims[axis_at] // parts).reshape((-1,) + (1,) * (len(dims) - axis_at - 1))

    factor_of = one(*pieces[0])
    for cut in pieces[1:]:
        factor_of = factor_of * one(*cut)
    return factor_of


def setup_inputs(seed: int = 0) -> dict:
    arg_keys = jax.random.split(jax.random.key(seed), 3)
    slab_pair = draw_slab_pair(jax.random.fold_in(arg_keys[2], 71), 0)
    butterfly_scale = jnp.clip(jnp.exp(math.log(2.0) - 1.3862944 * jax.random.uniform(arg_keys[1], (N,), jnp.float32) ** shard_levels(arg_keys[1], (N,), ((0, 4),), -0.2, 0.2)), 0.5, 2.0)
    return dict(slab_pair=slab_pair, butterfly_scale=butterfly_scale)


def reference(slab_pair, butterfly_scale):
    root_two = jnp.float32(2.0) ** 0.5
    upper = slab_pair[:HALF]
    lower = slab_pair[HALF:]
    rows_top = butterfly_scale[:HALF, None] * (upper + lower) / root_two
    rows_bottom = butterfly_scale[HALF:, None] * (upper - lower) / root_two
    rows_mixed = jnp.concatenate([rows_top, rows_bottom], axis=0)
    column_scale = jnp.concatenate([butterfly_scale[:W], butterfly_scale[HALF:HALF + W]])
    left_part = rows_mixed[:, :W]
    right_part = rows_mixed[:, W:]
    both_mixed = jnp.concatenate([left_part + right_part, left_part - right_part], axis=1)
    both_mixed = both_mixed * column_scale[None, :] / root_two
    row_index = jnp.arange(N, dtype=jnp.int32)[:, None]
    col_index = jnp.arange(2 * W, dtype=jnp.int32)[None, :]
    global_col = jnp.where(col_index < W, col_index, HALF + col_index - W)
    return jnp.where(row_index >= global_col, both_mixed, jnp.float32(0.0))
```

```python
import functools

import jax
import jax.numpy as jnp
from jax import lax
from jax.experimental import pallas as pl
from jax.experimental.pallas import tpu as pltpu
from jax.sharding import PartitionSpec as P

N = 65536
W = 2048
FULL_CHUNKS = 16
LANES = 128
AHEAD = 4
QUEUED = 2


def chunk_rows(local_rows):
    size = local_rows // FULL_CHUNKS
    sizes = [size // 4, size // 4, size // 2] + [size] * (FULL_CHUNKS - 1)
    starts = [sum(sizes[:k]) for k in range(len(sizes))]
    return list(zip(starts, sizes))


def routes(row_count, col_count):
    half_rows = row_count // 2
    half_cols = col_count // 2
    across = []
    for col in range(half_cols):
        across += [(col, col + half_cols), (col + half_cols, col)]
    down_up = []
    for row in range(half_rows):
        for col in range(col_count):
            top = row * col_count + col
            bottom = (row + half_rows) * col_count + col
            down_up.append((top, bottom))
            if col < half_cols:
                down_up.append((bottom, top))
    return across, down_up


def mix_kernel(here_ref, partner_ref, mixed_ref):
    is_left = lax.axis_index("col") < lax.axis_size("col") // 2
    sign = jnp.where(is_left, jnp.float32(1.0), jnp.float32(-1.0))
    mixed_ref[...] = partner_ref[...] + sign * here_ref[...]


def mix(slab_pair, partner, start, tile):
    size, cols = partner.shape
    first = start // tile
    return pl.pallas_call(
        mix_kernel,
        grid=(size // tile,),
        in_specs=[
            pl.BlockSpec((tile, cols), lambda i: (first + i, 0)),
            pl.BlockSpec((tile, cols), lambda i: (i, 0)),
        ],
        out_specs=pl.BlockSpec((tile, cols), lambda i: (i, 0)),
        out_shape=jax.ShapeDtypeStruct((size, cols), jnp.float32),
        cost_estimate=pl.CostEstimate(
            flops=2 * size * cols, bytes_accessed=12 * size * cols, transcendentals=0
        ),
        name="mix",
    )(slab_pair, partner)


def finish_kernel(start, tile, mixed_ref, other_ref, row_scale_ref, col_scale_ref, *rest):
    out_ref = rest[-1]
    local_rows = row_scale_ref.shape[0] * LANES
    local_cols = out_ref.shape[1]
    row_here = lax.axis_index("row")
    col_here = lax.axis_index("col")
    is_top = row_here < lax.axis_size("row") // 2
    sign = jnp.where(is_top, jnp.float32(1.0), jnp.float32(-1.0))
    step = pl.program_id(0)
    col_index = col_here * local_cols + lax.broadcasted_iota(jnp.int32, (LANES, local_cols), 1)
    global_col = jnp.where(col_index < W, col_index, N // 2 + col_index - W)
    row_offset = lax.broadcasted_iota(jnp.int32, (LANES, local_cols), 0)
    col_scale = col_scale_ref[0:1, :]
    for group in range(tile // LANES):
        rows = pl.ds(group * LANES, LANES)
        block = start // LANES + step * (tile // LANES) + group
        lane_scale = row_scale_ref[pl.ds(block, 1), :]
        row_scale = jnp.broadcast_to(lane_scale, (LANES, LANES)).T
        row_scale = jnp.concatenate([row_scale] * (local_cols // LANES), axis=1)
        both = other_ref[rows, :] + sign * mixed_ref[rows, :]
        both = both * row_scale * col_scale
        row_index = row_here * local_rows + block * LANES + row_offset
        out_ref[rows, :] = jnp.where(row_index >= global_col, both, jnp.float32(0.0))


def finish(out, mixed, other, row_scale, col_scale, later, start, tile, local_rows):
    size, cols = mixed.shape
    first = start // tile
    anywhere = pl.BlockSpec(memory_space=pl.ANY)
    in_specs = [
        pl.BlockSpec((tile, cols), lambda i: (i, 0)),
        pl.BlockSpec((tile, cols), lambda i: (i, 0)),
        pl.BlockSpec(row_scale.shape, lambda i: (0, 0)),
        pl.BlockSpec(col_scale.shape, lambda i: (0, 0)),
    ]
    operands = [mixed, other, row_scale, col_scale]
    if later is not None:
        operands.append(later)
        in_specs.append(anywhere)
    aliases = {}
    if out is not None:
        aliases = {len(operands): 0}
        operands.append(out)
        in_specs.append(anywhere)
    return pl.pallas_call(
        functools.partial(finish_kernel, start, tile),
        grid=(size // tile,),
        in_specs=in_specs,
        out_specs=pl.BlockSpec((tile, cols), lambda i: (first + i, 0)),
        out_shape=jax.ShapeDtypeStruct((local_rows, cols), jnp.float32),
        input_output_aliases=aliases,
        cost_estimate=pl.CostEstimate(
            flops=5 * size * cols, bytes_accessed=12 * size * cols, transcendentals=0
        ),
        name="finish",
    )(*operands)


def per_device(slab_pair, butterfly_scale):
    row_count = lax.axis_size("row")
    col_count = lax.axis_size("col")
    col_here = lax.axis_index("col")
    local_rows, local_cols = slab_pair.shape
    across, down_up = routes(row_count, col_count)
    chunks = chunk_rows(local_rows)
    tile = chunks[0][1]
    row_scale = butterfly_scale.reshape(local_rows // LANES, LANES)

    mixed, other, heres = [], [], []
    state = {"out": None, "done": 0, "col_scale": None}

    def make_col_scale():
        first, _ = lax.optimization_barrier((butterfly_scale[:W], mixed[1]))
        gathered = lax.all_gather(first, "row", axis=0, tiled=True)
        middle = row_count // 2 * W
        full_scale = jnp.concatenate([gathered[:W], gathered[middle : middle + W]])
        col_scale = lax.dynamic_slice_in_dim(full_scale, col_here * local_cols, local_cols, 0)
        col_scale = col_scale * jnp.float32(0.5)
        return jnp.broadcast_to(col_scale[None, :], (8, local_cols))

    def finish_next():
        k = state["done"]
        later = mixed[k + QUEUED] if k + QUEUED < len(chunks) else None
        if state["col_scale"] is None:
            state["col_scale"] = make_col_scale()
        state["out"] = finish(
            state["out"], mixed[k], other[k], row_scale, state["col_scale"], later,
            chunks[k][0], tile, local_rows,
        )
        state["done"] = k + 1

    partners = []

    def send_across(k):
        start, size = chunks[k]
        if k >= AHEAD:
            source, _ = lax.optimization_barrier((slab_pair, state["out"]))
        elif k >= 2:
            source, _ = lax.optimization_barrier((slab_pair, partners[k - 2]))
        else:
            source = slab_pair
        heres.append(lax.slice_in_dim(source, start, start + size, axis=0))
        partners.append(lax.ppermute(heres[k], "col", across))

    def send_down(k):
        mixed.append(mix(slab_pair, partners[k], chunks[k][0], tile))
        other.append(lax.ppermute(mixed[k], ("row", "col"), down_up))

    for k in range(len(chunks) + AHEAD):
        if k >= AHEAD:
            finish_next()
        if k < len(chunks):
            send_across(k)
        if k >= QUEUED - 1 and k - QUEUED + 1 < len(chunks):
            send_down(k - QUEUED + 1)
    return state["out"]


def solution(mesh):
    in_specs = (P("row", "col"), P("row"))
    out_specs = P("row", "col")
    return jax.shard_map(
        per_device, mesh=mesh, in_specs=in_specs, out_specs=out_specs, check_vma=False
    )
```

```python
import functools

import jax
import jax.numpy as jnp
from jax import lax
from jax.experimental import pallas as pl
from jax.experimental.pallas import tpu as pltpu
from jax.sharding import PartitionSpec as P

N = 65536
W = 2048
FULL_CHUNKS = 16
LANES = 128
AHEAD = 4
QUEUED = 2


def chunk_rows(local_rows):
    size = local_rows // FULL_CHUNKS
    ramp = [size // 4, size // 4, size // 2]
    sizes = ramp + [size] * (FULL_CHUNKS - 2) + ramp[::-1]
    starts = [sum(sizes[:k]) for k in range(len(sizes))]
    return list(zip(starts, sizes))


def routes(row_count, col_count):
    half_rows = row_count // 2
    half_cols = col_count // 2
    across = []
    for col in range(half_cols):
        across += [(col, col + half_cols), (col + half_cols, col)]
    down_up = []
    for row in range(half_rows):
        for col in range(col_count):
            top = row * col_count + col
            bottom = (row + half_rows) * col_count + col
            down_up.append((top, bottom))
            if col < half_cols:
                down_up.append((bottom, top))
    return across, down_up


def mix_kernel(here_ref, partner_ref, *rest):
    mixed_ref = rest[-1]
    is_left = lax.axis_index("col") < lax.axis_size("col") // 2
    sign = jnp.where(is_left, jnp.float32(1.0), jnp.float32(-1.0))
    mixed_ref[...] = partner_ref[...] + sign * here_ref[...]


def mix(slab_pair, partner, start, tile, earlier):
    size, cols = partner.shape
    first = start // tile
    anywhere = pl.BlockSpec(memory_space=pl.ANY)
    return pl.pallas_call(
        mix_kernel,
        grid=(size // tile,),
        in_specs=[
            pl.BlockSpec((tile, cols), lambda i: (first + i, 0)),
            pl.BlockSpec((tile, cols), lambda i: (i, 0)),
        ]
        + [anywhere] * len(earlier),
        out_specs=pl.BlockSpec((tile, cols), lambda i: (i, 0)),
        out_shape=jax.ShapeDtypeStruct((size, cols), jnp.float32),
        cost_estimate=pl.CostEstimate(
            flops=2 * size * cols, bytes_accessed=12 * size * cols, transcendentals=0
        ),
        name="mix",
    )(slab_pair, partner, *earlier)


def finish_kernel(start, tile, mixed_ref, other_ref, row_scale_ref, col_scale_ref, *rest):
    out_ref = rest[-1]
    local_rows = row_scale_ref.shape[0] * LANES
    local_cols = out_ref.shape[1]
    row_here = lax.axis_index("row")
    col_here = lax.axis_index("col")
    is_top = row_here < lax.axis_size("row") // 2
    sign = jnp.where(is_top, jnp.float32(1.0), jnp.float32(-1.0))
    step = pl.program_id(0)
    col_index = col_here * local_cols + lax.broadcasted_iota(jnp.int32, (LANES, local_cols), 1)
    global_col = jnp.where(col_index < W, col_index, N // 2 + col_index - W)
    row_offset = lax.broadcasted_iota(jnp.int32, (LANES, local_cols), 0)
    col_scale = col_scale_ref[0:1, :]
    for group in range(tile // LANES):
        rows = pl.ds(group * LANES, LANES)
        block = start // LANES + step * (tile // LANES) + group
        lane_scale = row_scale_ref[pl.ds(block, 1), :]
        row_scale = jnp.broadcast_to(lane_scale, (LANES, LANES)).T
        row_scale = jnp.concatenate([row_scale] * (local_cols // LANES), axis=1)
        both = other_ref[rows, :] + sign * mixed_ref[rows, :]
        both = both * row_scale * col_scale
        row_index = row_here * local_rows + block * LANES + row_offset
        out_ref[rows, :] = jnp.where(row_index >= global_col, both, jnp.float32(0.0))


def finish(out, mixed, other, row_scale, col_scale, later, start, tile, local_rows):
    size, cols = mixed.shape
    first = start // tile
    anywhere = pl.BlockSpec(memory_space=pl.ANY)
    in_specs = [
        pl.BlockSpec((tile, cols), lambda i: (i, 0)),
        pl.BlockSpec((tile, cols), lambda i: (i, 0)),
        pl.BlockSpec(row_scale.shape, lambda i: (0, 0)),
        pl.BlockSpec(col_scale.shape, lambda i: (0, 0)),
    ]
    operands = [mixed, other, row_scale, col_scale]
    if later is not None:
        operands.append(later)
        in_specs.append(anywhere)
    aliases = {}
    if out is not None:
        aliases = {len(operands): 0}
        operands.append(out)
        in_specs.append(anywhere)
    return pl.pallas_call(
        functools.partial(finish_kernel, start, tile),
        grid=(size // tile,),
        in_specs=in_specs,
        out_specs=pl.BlockSpec((tile, cols), lambda i: (first + i, 0)),
        out_shape=jax.ShapeDtypeStruct((local_rows, cols), jnp.float32),
        input_output_aliases=aliases,
        cost_estimate=pl.CostEstimate(
            flops=5 * size * cols, bytes_accessed=12 * size * cols, transcendentals=0
        ),
        name="finish",
    )(*operands)


def per_device(slab_pair, butterfly_scale):
    row_count = lax.axis_size("row")
    col_count = lax.axis_size("col")
    col_here = lax.axis_index("col")
    local_rows, local_cols = slab_pair.shape
    across, down_up = routes(row_count, col_count)
    chunks = chunk_rows(local_rows)
    tile = chunks[0][1]
    row_scale = butterfly_scale.reshape(local_rows // LANES, LANES)

    mixed, other, heres = [], [], []
    state = {"out": None, "done": 0, "col_scale": None}

    def make_col_scale():
        first, _ = lax.optimization_barrier((butterfly_scale[:W], heres[0]))
        gathered = lax.all_gather(first, "row", axis=0, tiled=True)
        middle = row_count // 2 * W
        full_scale = jnp.concatenate([gathered[:W], gathered[middle : middle + W]])
        col_scale = lax.dynamic_slice_in_dim(full_scale, col_here * local_cols, local_cols, 0)
        col_scale = col_scale * jnp.float32(0.5)
        state["col_scale"] = jnp.broadcast_to(col_scale[None, :], (8, local_cols))
        return state["col_scale"]

    def finish_next():
        k = state["done"]
        later = mixed[k + QUEUED] if k + QUEUED < len(chunks) else None
        state["out"] = finish(
            state["out"], mixed[k], other[k], row_scale, state["col_scale"], later,
            chunks[k][0], tile, local_rows,
        )
        state["done"] = k + 1

    partners = []

    def send_across(k):
        start, size = chunks[k]
        if k >= AHEAD:
            source, _ = lax.optimization_barrier((slab_pair, state["out"]))
        elif k >= 1:
            source, _ = lax.optimization_barrier((slab_pair, partners[k - 1]))
        else:
            source = slab_pair
        heres.append(lax.slice_in_dim(source, start, start + size, axis=0))
        partners.append(lax.ppermute(heres[k], "col", across))

    def send_down(k):
        earlier = [make_col_scale()] if k == 0 else []
        mixed.append(mix(slab_pair, partners[k], chunks[k][0], tile, earlier))
        other.append(lax.ppermute(mixed[k], ("row", "col"), down_up))

    for k in range(len(chunks) + AHEAD):
        if k >= AHEAD:
            finish_next()
        if k < len(chunks):
            send_across(k)
        if k >= QUEUED - 1 and k - QUEUED + 1 < len(chunks):
            send_down(k - QUEUED + 1)
    return state["out"]


def solution(mesh):
    in_specs = (P("row", "col"), P("row"))
    out_specs = P("row", "col")
    return jax.shard_map(
        per_device, mesh=mesh, in_specs=in_specs, out_specs=out_specs, check_vma=False
    )
```

```python
import functools

import jax
import jax.numpy as jnp
from jax import lax
from jax.experimental import pallas as pl
from jax.sharding import PartitionSpec as P

N = 65536
W = 2048
FULL_CHUNKS = 16
LANES = 128
AHEAD = 4
QUEUED = 2


def chunk_rows(local_rows):
    size = local_rows // FULL_CHUNKS
    ramp = [size // 4, size // 4, size // 2]
    sizes = ramp + [size] * (FULL_CHUNKS - 2) + ramp[::-1]
    starts = [sum(sizes[:k]) for k in range(len(sizes))]
    return list(zip(starts, sizes))


def routes(row_count, col_count):
    half_rows = row_count // 2
    half_cols = col_count // 2
    across = []
    for col in range(half_cols):
        across += [(col, col + half_cols), (col + half_cols, col)]
    down_up = []
    for row in range(half_rows):
        for col in range(col_count):
            top = row * col_count + col
            bottom = (row + half_rows) * col_count + col
            down_up.append((top, bottom))
            if col < half_cols:
                down_up.append((bottom, top))
    return across, down_up


def mix_kernel(here_ref, partner_ref, *rest):
    mixed_ref = rest[-1]
    is_left = lax.axis_index("col") < lax.axis_size("col") // 2
    sign = jnp.where(is_left, jnp.float32(1.0), jnp.float32(-1.0))
    mixed_ref[...] = partner_ref[...] + sign * here_ref[...]


def mix(slab_pair, partner, start, tile, earlier):
    size, cols = partner.shape
    first = start // tile
    anywhere = pl.BlockSpec(memory_space=pl.ANY)
    return pl.pallas_call(
        mix_kernel,
        grid=(size // tile,),
        in_specs=[
            pl.BlockSpec((tile, cols), lambda i: (first + i, 0)),
            pl.BlockSpec((tile, cols), lambda i: (i, 0)),
        ]
        + [anywhere] * len(earlier),
        out_specs=pl.BlockSpec((tile, cols), lambda i: (i, 0)),
        out_shape=jax.ShapeDtypeStruct((size, cols), jnp.float32),
        cost_estimate=pl.CostEstimate(
            flops=2 * size * cols, bytes_accessed=12 * size * cols, transcendentals=0
        ),
        name="mix",
    )(slab_pair, partner, *earlier)


def finish_kernel(start, tile, mixed_ref, other_ref, row_scale_ref, col_scale_ref, *rest):
    out_ref = rest[-1]
    local_rows = row_scale_ref.shape[0] * LANES
    local_cols = out_ref.shape[1]
    row_here = lax.axis_index("row")
    col_here = lax.axis_index("col")
    is_top = row_here < lax.axis_size("row") // 2
    sign = jnp.where(is_top, jnp.float32(1.0), jnp.float32(-1.0))
    step = pl.program_id(0)
    col_index = col_here * local_cols + lax.broadcasted_iota(jnp.int32, (LANES, local_cols), 1)
    global_col = jnp.where(col_index < W, col_index, N // 2 + col_index - W)
    row_offset = lax.broadcasted_iota(jnp.int32, (LANES, local_cols), 0)
    col_scale = col_scale_ref[0:1, :]
    for group in range(tile // LANES):
        rows = pl.ds(group * LANES, LANES)
        block = start // LANES + step * (tile // LANES) + group
        lane_scale = row_scale_ref[pl.ds(block, 1), :]
        row_scale = jnp.broadcast_to(lane_scale, (LANES, LANES)).T
        row_scale = jnp.concatenate([row_scale] * (local_cols // LANES), axis=1)
        both = other_ref[rows, :] + sign * mixed_ref[rows, :]
        both = both * row_scale * col_scale
        row_index = row_here * local_rows + block * LANES + row_offset
        out_ref[rows, :] = jnp.where(row_index >= global_col, both, jnp.float32(0.0))


def finish(out, mixed, other, row_scale, col_scale, later, start, tile, local_rows):
    size, cols = mixed.shape
    first = start // tile
    anywhere = pl.BlockSpec(memory_space=pl.ANY)
    in_specs = [
        pl.BlockSpec((tile, cols), lambda i: (i, 0)),
        pl.BlockSpec((tile, cols), lambda i: (i, 0)),
        pl.BlockSpec(row_scale.shape, lambda i: (0, 0)),
        pl.BlockSpec(col_scale.shape, lambda i: (0, 0)),
    ]
    operands = [mixed, other, row_scale, col_scale]
    if later is not None:
        operands.append(later)
        in_specs.append(anywhere)
    aliases = {}
    if out is not None:
        aliases = {len(operands): 0}
        operands.append(out)
        in_specs.append(anywhere)
    return pl.pallas_call(
        functools.partial(finish_kernel, start, tile),
        grid=(size // tile,),
        in_specs=in_specs,
        out_specs=pl.BlockSpec((tile, cols), lambda i: (first + i, 0)),
        out_shape=jax.ShapeDtypeStruct((local_rows, cols), jnp.float32),
        input_output_aliases=aliases,
        cost_estimate=pl.CostEstimate(
            flops=5 * size * cols, bytes_accessed=12 * size * cols, transcendentals=0
        ),
        name="finish",
    )(*operands)


def per_device(slab_pair, butterfly_scale):
    row_count = lax.axis_size("row")
    col_count = lax.axis_size("col")
    col_here = lax.axis_index("col")
    local_rows, local_cols = slab_pair.shape
    across, down_up = routes(row_count, col_count)
    chunks = chunk_rows(local_rows)
    tile = chunks[0][1]
    row_scale = butterfly_scale.reshape(local_rows // LANES, LANES)

    mixed, other, heres = [], [], []
    state = {"out": None, "done": 0, "col_scale": None}

    def make_col_scale():
        first, _ = lax.optimization_barrier((butterfly_scale[:W], heres[1]))
        gathered = lax.all_gather(first, "row", axis=0, tiled=True)
        middle = row_count // 2 * W
        full_scale = jnp.concatenate([gathered[:W], gathered[middle : middle + W]])
        col_scale = lax.dynamic_slice_in_dim(full_scale, col_here * local_cols, local_cols, 0)
        col_scale = col_scale * jnp.float32(0.5)
        state["col_scale"] = jnp.broadcast_to(col_scale[None, :], (8, local_cols))
        return state["col_scale"]

    def finish_next():
        k = state["done"]
        later = mixed[k + QUEUED] if k + QUEUED < len(chunks) else None
        state["out"] = finish(
            state["out"], mixed[k], other[k], row_scale, state["col_scale"], later,
            chunks[k][0], tile, local_rows,
        )
        state["done"] = k + 1

    partners = []

    def send_across(k):
        start, size = chunks[k]
        if k >= AHEAD:
            source, _ = lax.optimization_barrier((slab_pair, state["out"]))
        elif k >= 2:
            source, _ = lax.optimization_barrier((slab_pair, mixed[k - 2]))
        else:
            source = slab_pair
        heres.append(lax.slice_in_dim(source, start, start + size, axis=0))
        partners.append(lax.ppermute(heres[k], "col", across))

    def send_down(k):
        earlier = [make_col_scale()] if k == 0 else []
        mixed.append(mix(slab_pair, partners[k], chunks[k][0], tile, earlier))
        other.append(lax.ppermute(mixed[k], ("row", "col"), down_up))

    for k in range(len(chunks) + AHEAD):
        if k >= AHEAD:
            finish_next()
        if k < len(chunks):
            send_across(k)
        if k >= QUEUED - 1 and k - QUEUED + 1 < len(chunks):
            send_down(k - QUEUED + 1)
    return state["out"]


def solution(mesh):
    in_specs = (P("row", "col"), P("row"))
    out_specs = P("row", "col")

    return jax.shard_map(
        per_device, mesh=mesh, in_specs=in_specs, out_specs=out_specs, check_vma=False
    )
```

```python
import functools

import jax
import jax.numpy as jnp
from jax import lax
from jax.experimental import pallas as pl
from jax.sharding import PartitionSpec as P

N = 65536
W = 2048
FULL_CHUNKS = 16
LANES = 128
AHEAD = 4
QUEUED = 2
FIRST_CHUNK_AFTER = 3


def chunk_rows(local_rows):
    size = local_rows // FULL_CHUNKS
    ramp = [size // 4, size // 4, size // 2]
    sizes = ramp + [size] * (FULL_CHUNKS - 2) + ramp[::-1]
    starts = [sum(sizes[:k]) for k in range(len(sizes))]
    return list(zip(starts, sizes))


def routes(row_count, col_count):
    half_rows = row_count // 2
    half_cols = col_count // 2
    across = []
    for col in range(half_cols):
        across += [(col, col + half_cols), (col + half_cols, col)]
    down_up = []
    for row in range(half_rows):
        for col in range(col_count):
            top = row * col_count + col
            bottom = (row + half_rows) * col_count + col
            down_up.append((top, bottom))
            if col < half_cols:
                down_up.append((bottom, top))
    return across, down_up


def sign_along(axis):
    is_first = lax.axis_index(axis) < lax.axis_size(axis) // 2
    return jnp.where(is_first, jnp.float32(1.0), jnp.float32(-1.0))


def mix_kernel(axis, here_ref, partner_ref, mixed_ref):
    sign = sign_along(axis)
    mixed_ref[...] = partner_ref[...] + sign * here_ref[...]


def mix(axis, slab_pair, partner, start, tile):
    size, cols = partner.shape
    first = start // tile
    return pl.pallas_call(
        functools.partial(mix_kernel, axis),
        grid=(size // tile,),
        in_specs=[
            pl.BlockSpec((tile, cols), lambda i: (first + i, 0)),
            pl.BlockSpec((tile, cols), lambda i: (i, 0)),
        ],
        out_specs=pl.BlockSpec((tile, cols), lambda i: (i, 0)),
        out_shape=jax.ShapeDtypeStruct((size, cols), jnp.float32),
        cost_estimate=pl.CostEstimate(
            flops=2 * size * cols, bytes_accessed=12 * size * cols, transcendentals=0
        ),
        name="mix",
    )(slab_pair, partner)


def finish_kernel(axis, start, tile, mixed_ref, other_ref, row_scale_ref, col_scale_ref, *rest):
    out_ref = rest[-1]
    local_rows = row_scale_ref.shape[0] * LANES
    local_cols = out_ref.shape[1]
    row_here = lax.axis_index("row")
    col_here = lax.axis_index("col")
    sign = sign_along(axis)
    step = pl.program_id(0)
    col_index = col_here * local_cols + lax.broadcasted_iota(jnp.int32, (LANES, local_cols), 1)
    global_col = jnp.where(col_index < W, col_index, N // 2 + col_index - W)
    row_offset = lax.broadcasted_iota(jnp.int32, (LANES, local_cols), 0)
    col_scale = col_scale_ref[0:1, :]
    for group in range(tile // LANES):
        rows = pl.ds(group * LANES, LANES)
        block = start // LANES + step * (tile // LANES) + group
        lane_scale = row_scale_ref[pl.ds(block, 1), :]
        row_scale = jnp.broadcast_to(lane_scale, (LANES, LANES)).T
        row_scale = jnp.concatenate([row_scale] * (local_cols // LANES), axis=1)
        both = other_ref[rows, :] + sign * mixed_ref[rows, :]
        both = both * row_scale * col_scale
        row_index = row_here * local_rows + block * LANES + row_offset
        out_ref[rows, :] = jnp.where(row_index >= global_col, both, jnp.float32(0.0))


def finish(axis, out, mixed, other, row_scale, col_scale, later, start, tile, local_rows):
    size, cols = mixed.shape
    first = start // tile
    anywhere = pl.BlockSpec(memory_space=pl.ANY)
    in_specs = [
        pl.BlockSpec((tile, cols), lambda i: (i, 0)),
        pl.BlockSpec((tile, cols), lambda i: (i, 0)),
        pl.BlockSpec(row_scale.shape, lambda i: (0, 0)),
        pl.BlockSpec(col_scale.shape, lambda i: (0, 0)),
    ]
    operands = [mixed, other, row_scale, col_scale]
    if later is not None:
        operands.append(later)
        in_specs.append(anywhere)
    aliases = {}
    if out is not None:
        aliases = {len(operands): 0}
        operands.append(out)
        in_specs.append(anywhere)
    return pl.pallas_call(
        functools.partial(finish_kernel, axis, start, tile),
        grid=(size // tile,),
        in_specs=in_specs,
        out_specs=pl.BlockSpec((tile, cols), lambda i: (first + i, 0)),
        out_shape=jax.ShapeDtypeStruct((local_rows, cols), jnp.float32),
        input_output_aliases=aliases,
        cost_estimate=pl.CostEstimate(
            flops=5 * size * cols, bytes_accessed=12 * size * cols, transcendentals=0
        ),
        name="finish",
    )(*operands)


def column_scale(butterfly_scale, local_cols):
    row_count = lax.axis_size("row")
    col_count = lax.axis_size("col")
    half_rows = row_count // 2
    half_cols = col_count // 2
    row_here = lax.axis_index("row")
    col_here = lax.axis_index("col")
    place = lax.rem(col_here, half_cols) * local_cols
    mine = lax.dynamic_slice_in_dim(butterfly_scale, place, local_cols, 0)
    owner = jnp.where(col_here < half_cols, 0, half_rows)
    terms = [jnp.where(row_here == owner, mine, jnp.float32(0.0))]
    for step in range(1, row_count):
        route = []
        for col in range(col_count):
            source = 0 if col < half_cols else half_rows
            if source + step < row_count:
                route.append((source * col_count + col, (source + step) * col_count + col))
        terms.append(lax.ppermute(mine, ("row", "col"), route))
    return terms


def per_device(slab_pair, butterfly_scale):
    row_count = lax.axis_size("row")
    col_count = lax.axis_size("col")
    half_rows = row_count // 2
    local_rows, local_cols = slab_pair.shape
    across, down_up = routes(row_count, col_count)
    swap_rows = [(row, (row + half_rows) % row_count) for row in range(row_count)]
    chunks = chunk_rows(local_rows)
    count = len(chunks)
    tile = chunks[0][1]
    row_scale = butterfly_scale.reshape(local_rows // LANES, LANES)
    scale_terms = column_scale(butterfly_scale, local_cols)
    partners, mixed, other = {}, {}, {}
    out = None

    head = lax.slice_in_dim(slab_pair, 0, tile, axis=0)
    partners[0] = lax.ppermute(head, "row", swap_rows)
    mixed[0] = mix("row", slab_pair, partners[0], 0, tile)
    other[0] = lax.ppermute(mixed[0], "col", across)

    for k in range(1, count + AHEAD):
        done = k - AHEAD
        if done == 1:
            terms, _ = lax.optimization_barrier((scale_terms, mixed[1 + QUEUED]))
            total = sum(terms) * jnp.float32(0.5)
            col_scale = jnp.broadcast_to(total[None, :], (8, local_cols))
        if done >= 1:
            for j in [done, 0] if done == FIRST_CHUNK_AFTER else [done]:
                later = mixed.get(j + QUEUED) if j else None
                out = finish(
                    "row" if j else "col", out, mixed[j], other[j], row_scale, col_scale,
                    later, chunks[j][0], tile, local_rows,
                )
        if k < count:
            source = slab_pair
            if done >= 1:
                source, _ = lax.optimization_barrier((slab_pair, out))
            elif k >= 3:
                source, _ = lax.optimization_barrier((slab_pair, mixed[k - 2]))
            start, size = chunks[k]
            here = lax.slice_in_dim(source, start, start + size, axis=0)
            partners[k] = lax.ppermute(here, "col", across)
        if 1 <= k - 1 < count:
            j = k - 1
            mixed[j] = mix("col", slab_pair, partners[j], chunks[j][0], tile)
            other[j] = lax.ppermute(mixed[j], ("row", "col"), down_up)
    return out


def solution(mesh):
    in_specs = (P("row", "col"), P("row"))
    out_specs = P("row", "col")

    return jax.shard_map(
        per_device, mesh=mesh, in_specs=in_specs, out_specs=out_specs, check_vma=False
    )
```
